128 devices in a mesh: ga: 32 (over z, y, core), ba: 4 (over x).
Axes of the slice: x: 4, y: 4, z: 4, core: 2. Of those that a mesh axis runs over, the one named last changes fastest.
Arguments:
- coefficients: bfloat16 [40960, 6144], P('ga', 'ba')
- rotation: bfloat16 [6144, 6144], P('ga', 'ba'), may hold values from -0.078125 to 0.078125
Outputs:
- new_coefficients: bfloat16 [40960, 6144], P('ga', 'ba')
- band_rms: float32 [6144], P('ba')
The draws below stay inside these ranges and needn't reach their ends.
All inputs are finite; a program needn't handle non-finite values.
Results may differ from the reference program's by a relative error of at most 0.0004.
Values may be sent and summed in bfloat16 or wider, within the bound.
No kernel may reach another device: no remote copies, remote signals or barrier semaphores. Data moves between devices by JAX's collectives and lax.ppermute only.
A program may use at most 128 MiB of HBM per device.

```python
import math
import jax
import jax.numpy as jnp
from jax import lax

NB = 6144
NG = 40960


def draw_coefficients(key, part):
    first, second, third = jax.random.split(jax.random.fold_in(key, 11), 3)
    positions = jnp.arange(NG, dtype=jnp.float32)[:, None]
    row_scale = jnp.exp(positions / NG * math.log(3.0)) * jnp.exp(jax.random.uniform(first, (NG, 1), jnp.float32) * math.log(3.3))
    col_scale = jnp.exp(jax.random.uniform(second, (1, NB), jnp.float32) * math.log(10.0))
    base = jnp.clip(jax.random.normal(third, (NG, NB), jnp.float32), -6.0, 6.0)
    return (base * row_scale * col_scale).astype(jnp.bfloat16)


def steps_of(own_key, shape, shards, least, largest):
    loudness = 1.0
    for axis_at, parts in shards:
        heights = jax.random.uniform(jax.random.fold_in(jax.random.fold_in(own_key, 6), axis_at), (parts,), jnp.float32, least / len(shards), largest / len(shards))
        loudness = loudness * jnp.repeat(jnp.exp(heights), shape[axis_at] // parts).reshape((-1,) + (1,) * (len(shape) - 1 - axis_at))
    return loudness


def normal_values(own_key, shape, deviation, limit, shards=(), kind=jnp.bfloat16):
    drawn = jax.random.normal(own_key, shape, jnp.float32) * deviation
    if len(shards) > 0:
        drawn = steps_of(own_key, shape, shards, -0.22, 0.18) * drawn
    return jnp.clip(drawn, min=-limit, max=limit).astype(kind)


def setup_inputs(seed: int = 0) -> dict:
    seeds = jax.random.split(jax.random.key(seed), 3)
    coefficients = draw_coefficients(jax.random.fold_in(seeds[2], 71), 0)
    rotation = normal_values(seeds[1], (NB, NB), NB ** -0.5, 0.078125, ((0, 32), (1, 4)))
    return {"coefficients": coefficients, "rotation": rotation}


def reference(coefficients, rotation):
    rotated = jnp.dot(coefficients, rotation, preferred_element_type=jnp.float32)
    sums = lax.optimization_barrier(jnp.sum(rotated * rotated, axis=0))
    band_rms = jnp.sqrt(sums / NG + 1e-06)
    return ((rotated / band_rms).astype(jnp.bfloat16), band_rms)
```

```python
import functools

import jax
import jax.numpy as jnp
from jax import lax
from jax.experimental import pallas as pl
from jax.experimental.pallas import tpu as pltpu
from jax.sharding import PartitionSpec as P


LAST = 128
OFFSETS = (0, -1, 1, 2)


def plane(shift_of):
    pairs = []
    for z in range(4):
        for y in range(4):
            for c in range(2):
                tz, ty, tc = shift_of(z, y, c)
                pairs.append((z * 8 + y * 2 + c, (tz % 4) * 8 + (ty % 4) * 2 + tc))
    return pairs


def first_axis(step):
    return plane(lambda z, y, c: (z, y + step, c) if c == 0 else (z + step, y, c))


def second_axis(step):
    return plane(lambda z, y, c: (z + step, y, c) if c == 0 else (z, y + step, c))


def gather4(own, ring):
    half = own.shape[0] // 2
    left = lax.ppermute(own, "ga", ring(1))
    right = lax.ppermute(own, "ga", ring(-1))
    far_a = lax.ppermute(left[:half], "ga", ring(1))
    far_b = lax.ppermute(right[half:], "ga", ring(-1))
    return [own, left, right, far_a, far_b]


def piece_offsets(pieces, sub):
    found = []
    for array, offset, base in zip(range(5), (0, -1, 1, 2, 2), (0, 0, 0, 0, 2)):
        for j in range(pieces[array].shape[0] // sub):
            found.append((array, j * sub, offset, OFFSETS[base + j]))
    return found


def first_kernel(layout, sub, *refs):
    n_r = 10
    r_refs, (own, l0, l1, r0, r1) = refs[:n_r], refs[n_r : n_r + 5]
    total, r_far, r_all, a_all, r_sem, a_sem = refs[n_r + 5 :]
    ga, x = lax.axis_index("ga"), lax.axis_index("ba")
    z, y, c = ga // 8, (ga // 2) % 4, ga % 2
    depth = own.shape[1]
    half = l0.shape[0]
    copies = []
    for which in range(2):
        core = c if which == 0 else 1 - c
        for array, row, near, far in layout:
            zz = jnp.where(core == 0, z + near, z + far)
            yy = jnp.where(core == 0, y + far, y + near)
            zz, yy = (zz + 4) % 4, (yy + 4) % 4
            slot = (zz - x + 5) % 4
            at = pl.multiple_of(slot * depth + (yy * 2 + core) * sub, 64)
            copies.append(
                pltpu.make_async_copy(
                    r_refs[which * 5 + array].at[pl.ds(row, sub)],
                    r_all.at[pl.ds(at, sub)],
                    r_sem,
                )
            )
    for ref, row, col in ((l0, 0, 0), (l1, half, 0), (own, 0, depth), (r0, 0, 2 * depth), (r1, half, 2 * depth)):
        copies.append(
            pltpu.make_async_copy(
                ref, a_all.at[pl.ds(row, ref.shape[0]), pl.ds(col, depth)], a_sem
            )
        )
    for copy in copies:
        copy.start()
    for copy in copies:
        copy.wait()
    r_far[...] = r_all[3 * depth :]
    tm, tn = 256, 512
    n_n = total.shape[1] // tn

    def tile(i, carry):
        rows = pl.ds(pl.multiple_of((i // n_n) * tm, tm), tm)
        cols = pl.ds(pl.multiple_of((i % n_n) * tn, tn), tn)
        total[rows, cols] = jnp.dot(
            a_all[rows, :], r_all[: 3 * depth, cols], preferred_element_type=jnp.float32
        )
        return carry

    lax.fori_loop(0, (total.shape[0] // tm) * n_n, tile, 0)


def last_kernel(tops, r_far, before, *refs):
    top, bottom, total_in, total, squares = refs[0], refs[1], refs[3], refs[4], refs[5]
    del r_far, before, total_in
    r = refs[2]
    tm, tn = 128, 512
    n_n = total.shape[1] // tn
    squares[...] = jnp.zeros_like(squares)
    for piece, start in zip((top, bottom), tops):

        def tile(i, carry, piece=piece, start=start):
            cols = pl.ds(pl.multiple_of((i % n_n) * tn, tn), tn)
            row = pl.multiple_of((i // n_n) * tm, tm)
            rows = pl.ds(pl.multiple_of(start + row, tm), tm)
            value = total[rows, cols] + jnp.dot(
                piece[pl.ds(row, tm), :], r[:, cols], preferred_element_type=jnp.float32
            )
            total[rows, cols] = value
            squares[:, cols] += jnp.sum((value * value).reshape(tm // 8, 8, tn), axis=0)
            return carry

        lax.fori_loop(0, (piece.shape[0] // tm) * n_n, tile, 0)


def normalize_kernel(count, total, everyone, new, band_rms, out, sem):
    squares = jnp.sum(everyone[...], axis=0, keepdims=True)
    rms = jnp.sqrt(squares / count + 1e-06)
    band_rms[...] = rms
    inverse = 1.0 / rms
    tm = 128
    steps = total.shape[0] // tm

    def copy(i):
        rows = pl.ds(pl.multiple_of(i * tm, tm), tm)
        return pltpu.make_async_copy(out.at[rows], new.at[rows], sem)

    def tile(i, carry):
        rows = pl.ds(pl.multiple_of(i * tm, tm), tm)
        out[rows, :] = (total[rows, :] * inverse).astype(out.dtype)
        copy(i).start()
        return carry

    lax.fori_loop(0, steps, tile, 0)
    pltpu.make_async_copy(out, new, sem).wait()


def finish(top, bottom, r_far, total, tops):
    rows, columns = total.shape
    vmem = pl.BlockSpec(memory_space=pltpu.VMEM)
    return pl.pallas_call(
        functools.partial(last_kernel, tops, None, None),
        out_shape=(
            jax.ShapeDtypeStruct((rows, columns), jnp.float32),
            jax.ShapeDtypeStruct((8, columns), jnp.float32),
        ),
        in_specs=[vmem] * 4,
        out_specs=(vmem, vmem),
        input_output_aliases={3: 0},
        cost_estimate=pl.CostEstimate(
            flops=2 * 2 * top.shape[0] * r_far.shape[0] * columns,
            bytes_accessed=4 * top.shape[0] * columns,
            transcendentals=0,
        ),
        compiler_params=pltpu.CompilerParams(vmem_limit_bytes=24 * 2**20),
    )(top, bottom, r_far, total)


def program(a, r):
    rows, depth = a.shape
    columns = r.shape[1]
    sub = r.shape[0]
    half = rows // 2
    to_right = [(i, (i + 1) % 4) for i in range(4)]
    to_left = [(i, (i + 3) % 4) for i in range(4)]
    top, bottom = a[:half], a[half:]

    l0 = lax.ppermute(top, "ba", to_right)
    r1 = lax.ppermute(bottom, "ba", to_left)
    l1 = lax.ppermute(bottom, "ba", to_right)
    r0 = lax.ppermute(top, "ba", to_left)
    cut = half - LAST
    far_t0 = lax.ppermute(l0[:cut], "ba", to_right)
    far_b0 = lax.ppermute(r1[:cut], "ba", to_left)
    far_t1 = lax.ppermute(l0[cut:], "ba", to_right)
    far_b1 = lax.ppermute(r1[cut:], "ba", to_left)

    inner = gather4(r, first_axis)
    ring = gather4(jnp.concatenate(inner, axis=0), second_axis)
    swap = plane(lambda z, y, c: (z, y, 1 - c))
    other = [lax.ppermute(piece, "ga", swap) for piece in ring]

    layout = piece_offsets(ring, sub)
    any_space = pl.BlockSpec(memory_space=pl.ANY)
    vmem = pl.BlockSpec(memory_space=pltpu.VMEM)
    total, r_far = pl.pallas_call(
        functools.partial(first_kernel, layout, sub),
        out_shape=(
            jax.ShapeDtypeStruct((rows, columns), jnp.float32),
            jax.ShapeDtypeStruct((depth, columns), jnp.bfloat16),
        ),
        in_specs=[any_space] * 15,
        out_specs=(vmem, vmem),
        scratch_shapes=[
            pltpu.VMEM((4 * depth, columns), jnp.bfloat16),
            pltpu.VMEM((rows, 3 * depth), jnp.bfloat16),
            pltpu.SemaphoreType.DMA,
            pltpu.SemaphoreType.DMA,
        ],
        cost_estimate=pl.CostEstimate(
            flops=2 * rows * 3 * depth * columns,
            bytes_accessed=2 * (rows * 3 * depth + 4 * depth * columns),
            transcendentals=0,
        ),
        compiler_params=pltpu.CompilerParams(vmem_limit_bytes=42 * 2**20),
        name="first",
    )(*ring, *other, a, l0, l1, r0, r1)
    total, squares_a = finish(far_t0, far_b0, r_far, total, (0, half))
    total, squares_b = finish(far_t1, far_b1, r_far, total, (cut, half + cut))
    squares = jnp.sum(squares_a + squares_b, axis=0)
    n = lax.axis_size("ga")
    everyone = lax.all_to_all(
        jnp.broadcast_to(squares, (n, 1, columns)), "ga", split_axis=0, concat_axis=0, tiled=True
    )
    new, band_rms = pl.pallas_call(
        functools.partial(normalize_kernel, rows * n),
        out_shape=(
            jax.ShapeDtypeStruct((rows, columns), jnp.bfloat16),
            jax.ShapeDtypeStruct((1, columns), jnp.float32),
        ),
        in_specs=[vmem, vmem],
        out_specs=(any_space, vmem),
        scratch_shapes=[
            pltpu.VMEM((rows, columns), jnp.bfloat16),
            pltpu.SemaphoreType.DMA,
        ],
        cost_estimate=pl.CostEstimate(
            flops=2 * rows * columns, bytes_accessed=6 * rows * columns, transcendentals=0
        ),
        compiler_params=pltpu.CompilerParams(vmem_limit_bytes=24 * 2**20),
        name="normalize",
    )(total, everyone.reshape(n, columns))
    return new, band_rms.reshape(columns)


def solution(mesh):
    in_specs = (P("ga", "ba"), P("ga", "ba"))
    out_specs = (P("ga", "ba"), P("ba"))
    return jax.shard_map(program, mesh=mesh, in_specs=in_specs, out_specs=out_specs, check_vma=False)
```
